128 devices in a mesh: ay: 8 (over x, core), ax: 16 (over y, z).
Axes of the slice: x: 4, y: 4, z: 4, core: 2. Of those that a mesh axis runs over, the one named last changes fastest.
Arguments:
- gaseous_model: float32 [4, 4096, 4096], P(None, 'ay', 'ax'), may hold values from -6 to 6
- forcing_boundary: float32 [4, 4096, 4096], P(None, 'ay', 'ax'), may hold values from -16 to 16, as said below
- relaxation_strength_profile: float32 [4], replicated, may hold values from 0.2 to 1
- bottom_exchange_aloft: bfloat16 [8, 4096, 4096], P(None, 'ay', 'ax'), may hold values from -6 to 6
- exchange_bottom_sensitivity: float32 [8], replicated, may hold values from -1 to 1
- terrain_skin_warmth: bfloat16 [4096, 4096], P('ay', 'ax'), may hold values from -6 to 6
- tile_processor_home: int32 [16384], replicated, may hold values from 0 to 128, as said below
- marine_place_warmth: float32 [16384, 2304], P(('ay', 'ax')), may hold values from -6 to 6
- warming_coefficient: float32 [8], replicated, may hold values from -0.5 to 0.5
Outputs:
- atmosphere_out: float32 [4, 4096, 4096], P(None, 'ay', 'ax')
- ocean_flux: bfloat16 [16384, 8, 2304], P(('ay', 'ax'))
- ocean_sst_out: float32 [16384, 2304], P(('ay', 'ax'))
- surface_temp: float32 [4096, 4096], P('ay', 'ax')
The draws below stay inside these ranges and needn't reach their ends.
Inputs may be any that keep to these rules, and one draw needn't show every extreme that they name: `forcing_boundary`: smooth large-scale patterns with cell-to-cell noise. `tile_processor_home`: 128 marks an all-land block that no ocean device holds. Among the 128 blocks of one tile at most 2 have the same owner, and some tile has exactly 2 with one owner. An ocean device holds at most 128 blocks, and some device holds exactly 128.
All inputs are finite; a program needn't handle non-finite values.
Results may differ from the reference program's by a relative error of at most 0.0037.
Values may be sent and summed in bfloat16 or wider, within the bound.
No kernel may reach another device: no remote copies, remote signals or barrier semaphores. Data moves between devices by JAX's collectives and lax.ppermute only.
A program may use at most 192 MiB of HBM per device.

```python
import math
import jax
import jax.numpy as jnp
from jax import lax

GRID = 4096
KMAX = 32
LEVELS = 4
EXCHANGE_KINDS = 8
ABLOCK = 32
MARINE_TILE_EDGE = 48
GAS_PATCH_TOTAL = 1024
MARINE_PATCHES = 2304
BLK_DEV = 128
CAP = 2
UNIT_PLACES = 128
N_AY = 8
N_AX = 16
DEVICES = 128


def wave_table(length, waves_top):
    points = jnp.arange(length, dtype=jnp.int32)
    wavenumbers = jnp.arange(1, waves_top + 1, dtype=jnp.int32)
    phases = points[:, None] * wavenumbers[None, :] % length
    angles = phases.astype(jnp.float32) * (2.0 * math.pi / length)
    constant = jnp.full((length, 1), math.sqrt(1.0 / length), jnp.float32)
    factor = math.sqrt(2.0 / length)
    return jnp.concatenate([constant, factor * jnp.cos(angles), factor * jnp.sin(angles)], axis=1)


def draw_forcing_boundary(key, part):
    key_smooth, key_noise = jax.random.split(jax.random.fold_in(key, 11), 2)
    harmonics = wave_table(GRID, KMAX)
    mode_count = 2 * KMAX + 1
    amplitude = jax.random.normal(key_smooth, (LEVELS, mode_count, mode_count), jnp.float32) * (GRID / mode_count)
    noise_part = 0.5 * jax.random.normal(key_noise, (LEVELS, GRID, GRID), jnp.float32)
    smooth = jnp.einsum('ym,lmn,xn->lyx', harmonics, amplitude, harmonics)
    return jnp.clip(smooth + noise_part, -16.0, 16.0)


def draw_tile_processor_home(key, part):
    key_order, key_shift, key_local, key_land = jax.random.split(jax.random.fold_in(key, 23), 4)
    groups = BLK_DEV // CAP
    owner_order = jax.random.permutation(key_order, DEVICES).astype(jnp.int32)
    group_shift = jax.random.permutation(key_shift, DEVICES).astype(jnp.int32)[:groups]
    device_keys = jax.random.split(key_local, DEVICES)
    shuffled = jax.vmap(lambda single: jax.random.permutation(single, BLK_DEV))(device_keys).astype(jnp.int32)
    group_of = shuffled // CAP
    source = jnp.arange(DEVICES, dtype=jnp.int32)[:, None]
    owner_rank = (source + group_shift[group_of]) % DEVICES
    owner_of = owner_order[owner_rank]
    land_level = owner_rank * 4 // DEVICES
    land_draw = jax.random.randint(key_land, (DEVICES, BLK_DEV), 0, 8, jnp.int32)
    is_wet = land_draw >= land_level
    return jnp.where(is_wet, owner_of, DEVICES).reshape(-1).astype(jnp.int32)


def block_scale(stream_key, extent, pieces, smallest, top_value):
    gain, own = 1.0, jax.random.fold_in(stream_key, 6)
    for dim, blocks in pieces:
        draws = jnp.exp(jax.random.uniform(jax.random.fold_in(own, dim), (blocks,), jnp.float32, smallest / len(pieces), top_value / len(pieces)))
        gain = gain * jnp.repeat(draws, extent[dim] // blocks).reshape([-1 if axis == dim else 1 for axis in range(len(extent))])
    return gain


def normal_values(own_key, dims, width, limit, cuts=(), kind=jnp.bfloat16):
    level = block_scale(own_key, dims, cuts, -0.22, 0.18) if cuts else 1.0
    entries = jax.random.normal(own_key, dims, jnp.float32) * width * level
    return jnp.minimum(jnp.maximum(entries, -limit), limit).astype(kind)


def setup_inputs(seed: int = 0) -> dict:
    arg_keys = jax.random.split(jax.random.key(seed), 10)
    gaseous_model = normal_values(arg_keys[0], (LEVELS, GRID, GRID), 1.0, 6.0, ((1, 8), (2, 16)), jnp.float32)
    forcing_boundary = draw_forcing_boundary(jax.random.fold_in(arg_keys[9], 71), 0)
    relaxation_strength_profile = jnp.clip(jnp.exp(jax.random.uniform(arg_keys[2], (LEVELS,), jnp.float32, math.log(0.2), math.log(1.0))), 0.2, 1.0)
    bottom_exchange_aloft = normal_values(arg_keys[3], (EXCHANGE_KINDS, GRID, GRID), 1.0, 6.0, ((1, 8), (2, 16)))
    exchange_bottom_sensitivity = jnp.clip(jax.random.uniform(arg_keys[4], (EXCHANGE_KINDS,), jnp.float32, -1.0, 1.0), -1.0, 1.0)
    terrain_skin_warmth = normal_values(arg_keys[5], (GRID, GRID), 1.0, 6.0, ((0, 8), (1, 16)))
    tile_processor_home = draw_tile_processor_home(jax.random.fold_in(arg_keys[9], 71), 0)
    marine_place_warmth = normal_values(arg_keys[7], (DEVICES * UNIT_PLACES, MARINE_PATCHES), 1.0, 6.0, ((0, 128),), jnp.float32)
    warming_coefficient = jnp.clip(jax.random.uniform(arg_keys[8], (EXCHANGE_KINDS,), jnp.float32, -0.5, 0.5), -0.5, 0.5)
    return dict(gaseous_model=gaseous_model, forcing_boundary=forcing_boundary, relaxation_strength_profile=relaxation_strength_profile, bottom_exchange_aloft=bottom_exchange_aloft, exchange_bottom_sensitivity=exchange_bottom_sensitivity, terrain_skin_warmth=terrain_skin_warmth, tile_processor_home=tile_processor_home, marine_place_warmth=marine_place_warmth, warming_coefficient=warming_coefficient)


highest_accuracy = lax.Precision.HIGHEST

def spectral_basis(length, offset, number, waves_top):
    points = offset + jnp.arange(number, dtype=jnp.int32)
    wavenumbers = jnp.arange(1, waves_top + 1, dtype=jnp.int32)
    phases = points[:, None] * wavenumbers[None, :] % length
    angles = phases.astype(jnp.float32) * (2.0 * math.pi / length)
    constant = jnp.full((number, 1), math.sqrt(1.0 / length), jnp.float32)
    factor = math.sqrt(2.0 / length)
    return jnp.concatenate([constant, factor * jnp.cos(angles), factor * jnp.sin(angles)], axis=1)

def intersection_table():
    ocean_index = jnp.arange(MARINE_TILE_EDGE, dtype=jnp.int32)[:, None]
    air_index = jnp.arange(ABLOCK, dtype=jnp.int32)[None, :]
    upper_edge = jnp.minimum(2 * ocean_index + 2, 3 * air_index + 3)
    lower_edge = jnp.maximum(2 * ocean_index, 3 * air_index)
    return jnp.maximum(upper_edge - lower_edge, 0).astype(jnp.float32)

def reference(gaseous_model, forcing_boundary, relaxation_strength_profile, bottom_exchange_aloft, exchange_bottom_sensitivity, terrain_skin_warmth, tile_processor_home, marine_place_warmth, warming_coefficient):
    harmonics = spectral_basis(GRID, 0, GRID, KMAX)
    departure = forcing_boundary - gaseous_model
    along_cols = jnp.einsum('lyx,xn->lyn', departure, harmonics, precision=highest_accuracy)
    coefficients = jnp.einsum('ym,lyn->lmn', harmonics, along_cols, precision=highest_accuracy)
    rows_back = jnp.einsum('ym,lmn->lyn', harmonics, coefficients, precision=highest_accuracy)
    filtered = jnp.einsum('lyn,xn->lyx', rows_back, harmonics, precision=highest_accuracy)
    advanced_condition = gaseous_model + relaxation_strength_profile[:, None, None] * filtered
    flux_air = (bottom_exchange_aloft.astype(jnp.float32) + exchange_bottom_sensitivity[:, None, None] * advanced_condition[LEVELS - 1]).astype(jnp.bfloat16)
    tile_rows = GRID // N_AY
    tile_cols = GRID // N_AX
    block_rows = tile_rows // ABLOCK
    block_cols = tile_cols // ABLOCK
    processor_portion = block_rows * block_cols
    processor_roster = N_AY * N_AX
    block_total = processor_roster * processor_portion
    blocks = flux_air.reshape(EXCHANGE_KINDS, N_AY, block_rows, ABLOCK, N_AX, block_cols, ABLOCK)
    blocks = blocks.transpose(1, 4, 2, 5, 0, 3, 6).reshape(block_total, EXCHANGE_KINDS, ABLOCK, ABLOCK)
    is_wet = tile_processor_home < processor_roster
    one_hot = (tile_processor_home[:, None] == jnp.arange(processor_roster + 1, dtype=jnp.int32)[None, :]).astype(jnp.int32)
    ranking = lax.optimization_barrier(jnp.sum((jnp.cumsum(one_hot, axis=0) - one_hot) * one_hot, axis=1)).astype(jnp.int32)
    numbers = jnp.arange(block_total, dtype=jnp.int32)
    slot_index = jnp.where(is_wet, tile_processor_home * processor_portion + ranking, processor_roster * processor_portion).astype(jnp.int32)
    place_tile_position = jnp.full((processor_roster * processor_portion,), block_total, jnp.int32).at[slot_index].set(numbers, mode='drop')
    forward_weights = intersection_table() / 2.0
    backward_coefficients = intersection_table() / 3.0

    def marine_labour(given_tensors):
        picked_option, marine_warmth_lines = given_tensors
        possessed_indicator = picked_option < block_total
        picked = blocks[jnp.minimum(picked_option, block_total - 1)].astype(jnp.float32)
        regrid = jnp.einsum('oa,sfac,pc->sfop', forward_weights, picked, forward_weights, precision=highest_accuracy)
        marine_exchange_mesh = jnp.where(possessed_indicator[:, None, None, None], regrid, 0.0).astype(jnp.bfloat16)
        marine_exchange_mesh = marine_exchange_mesh.reshape(processor_portion, EXCHANGE_KINDS, MARINE_PATCHES)
        marine_warming = jnp.einsum('f,sfk->sk', warming_coefficient, marine_exchange_mesh.astype(jnp.float32), precision=highest_accuracy)
        renewed_marine_warmth = jnp.where(possessed_indicator[:, None], marine_warmth_lines + marine_warming, 0.0)
        sent_back_entries = jnp.einsum('en,oea,am->onm', backward_coefficients, renewed_marine_warmth.reshape(processor_portion, MARINE_TILE_EDGE, MARINE_TILE_EDGE), backward_coefficients, precision=highest_accuracy)
        return (marine_exchange_mesh, renewed_marine_warmth, sent_back_entries.reshape(processor_portion, GAS_PATCH_TOTAL))
    exchange_outcome, marine_warmth_product, sent_back_entries = lax.map(marine_labour, (place_tile_position.reshape(processor_roster, processor_portion), marine_place_warmth.reshape(processor_roster, processor_portion, MARINE_PATCHES)))
    returned_flat = sent_back_entries.reshape(processor_roster * processor_portion, GAS_PATCH_TOTAL)
    position = jnp.where(is_wet, tile_processor_home * processor_portion + ranking, 0).astype(jnp.int32)
    air_blocks = returned_flat[position]
    land_blocks = terrain_skin_warmth.reshape(N_AY, block_rows, ABLOCK, N_AX, block_cols, ABLOCK)
    land_blocks = land_blocks.transpose(0, 3, 1, 4, 2, 5).reshape(block_total, GAS_PATCH_TOTAL).astype(jnp.float32)
    surface_blocks = jnp.where(is_wet[:, None], air_blocks, land_blocks)
    bottom_quantity = surface_blocks.reshape(N_AY, N_AX, block_rows, block_cols, ABLOCK, ABLOCK)
    bottom_quantity = bottom_quantity.transpose(0, 2, 4, 1, 3, 5).reshape(GRID, GRID)
    return (advanced_condition, exchange_outcome.reshape(processor_roster * processor_portion, EXCHANGE_KINDS, MARINE_PATCHES), marine_warmth_product.reshape(processor_roster * processor_portion, MARINE_PATCHES), bottom_quantity)
```

```python
import functools
import math

import jax
import jax.numpy as jnp
import numpy as np
from jax import lax
from jax.experimental import pallas as pl
from jax.experimental.pallas import tpu as pltpu
from jax.sharding import PartitionSpec as P

GRID = 4096
KMAX = 32
LEVELS = 4
FIELDS = 8
ABLOCK = 32
OBLOCK = 48
ACELLS = 1024
OCELLS = 2304
TILE_ROWS = 512
TILE_COLS = 256
BLOCK_ROWS = 16
BLOCK_COLS = 8
N_AX = 16
DEVICES = 128
SLOTS = 128
MODES = 64
CROWS = 72
MSG_ROWS = 72
F32 = jnp.float32
BF16 = jnp.bfloat16


def _split(x):
    hi = np.asarray(x, np.float32).astype(jnp.bfloat16)
    lo = (np.asarray(x, np.float64) - hi.astype(np.float64)).astype(jnp.bfloat16)
    return hi, lo


def _modes(points):
    k = np.arange(1, KMAX + 1)
    angle = (np.asarray(points)[:, None] * k[None, :] % GRID) * (2.0 * math.pi / GRID)
    factor = math.sqrt(2.0 / GRID)
    return np.concatenate([factor * np.cos(angle), factor * np.sin(angle)], axis=1)


def _intersection():
    o = np.arange(OBLOCK)[:, None]
    a = np.arange(ABLOCK)[None, :]
    return np.maximum(np.minimum(2 * o + 2, 3 * a + 3) - np.maximum(2 * o, 3 * a), 0).astype(np.float64)


@functools.cache
def _tables():
    hi, lo = _split(_modes(np.arange(GRID)))
    basis = np.concatenate([hi, lo], axis=1)
    inter = _intersection()
    kron = np.kron(inter, inter)
    forward = np.zeros((5, 256, 256), np.float32)
    for t, first in enumerate(FWD_FIRST):
        out = min(256, 1152 - 256 * t)
        forward[t, :, :out] = kron[256 * t : 256 * t + out, 128 * first : 128 * first + 256].T / 4.0
    back = np.zeros((4, 384, 128), np.float32)
    for j in range(4):
        back[j] = kron[256 * j : 256 * j + 384, 128 * j : 128 * j + 128]
    local = np.zeros((256, 128))
    for k in range(4):
        local[64 * k : 64 * k + 64, 32 * k : 32 * k + 32] = _modes(np.arange(ABLOCK)).T
    lhi, llo = _split(local)
    synth = np.concatenate([lhi, llo], axis=1)
    k = np.arange(1, KMAX + 1)
    alpha = (np.arange(128)[:, None] * ABLOCK * k[None, :] % GRID) * (2.0 * math.pi / GRID)
    c, s = np.cos(alpha), np.sin(alpha)
    turn = np.concatenate([c, c, c, c, s, -s, s, -s], axis=1).astype(np.float32)
    return basis, forward.astype(jnp.bfloat16), back.astype(jnp.bfloat16), synth, turn


FWD_FIRST = (0, 0, 1, 2, 2)


def _hilo(x):
    hi = x.astype(BF16)
    return hi, (x - hi.astype(F32)).astype(BF16)


def _mm(a, b):
    return jnp.dot(a, b, preferred_element_type=F32)


def _swap_groups(v, group):
    low2, even = group < 2, group % 2 == 0
    r = lambda x, n: pltpu.roll(x, n, 1)
    a0 = jnp.where(low2, v[0], r(v[2], 64))
    a2 = jnp.where(low2, r(v[0], 64), v[2])
    a1 = jnp.where(low2, v[1], r(v[3], 64))
    a3 = jnp.where(low2, r(v[1], 64), v[3])
    return (
        jnp.where(even, a0, r(a1, 32)),
        jnp.where(even, r(a0, 96), a1),
        jnp.where(even, a2, r(a3, 32)),
        jnp.where(even, r(a2, 96), a3),
    )


def _lane_group():
    return lax.broadcasted_iota(jnp.int32, (8, 128), 1) // 32


def _index_rows(owners, own, dev):
    lane = lax.broadcasted_iota(jnp.int32, (128, 128), 1)
    row = lax.broadcasted_iota(jnp.int32, (128, 128), 0)
    mine = owners == dev
    eq = mine.astype(F32)
    count = jnp.sum(eq, axis=1, keepdims=True)
    running = jnp.sum(_mm((row >= lane).astype(BF16), eq.astype(BF16)), axis=1, keepdims=True)
    before = (running <= lane.astype(F32)).astype(F32)
    tile = jnp.sum(before, axis=0, keepdims=True)
    base = jnp.sum(before * count, axis=0, keepdims=True)
    first = jnp.min(jnp.where(mine, lane, 127), axis=1, keepdims=True).astype(F32)
    last = jnp.max(jnp.where(mine, lane, 0), axis=1, keepdims=True).astype(F32)
    chosen = (row.astype(F32) == tile).astype(F32)
    first = jnp.sum(chosen * first, axis=0, keepdims=True)
    last = jnp.sum(chosen * last, axis=0, keepdims=True)
    tile_i = tile.astype(jnp.int32)
    nth = lane[:1] - base.astype(jnp.int32)
    held = tile_i < 128
    block = jnp.where(nth == 0, first, last).astype(jnp.int32)
    arrival = jnp.where(held, 2 * tile_i + nth, 0)
    block_row = jnp.where(held, (tile_i // N_AX) * BLOCK_ROWS + block // BLOCK_COLS, 0)
    block_col = jnp.where(held, (tile_i % N_AX) * BLOCK_COLS + block % BLOCK_COLS, 0)
    total = jnp.sum(held.astype(jnp.int32), axis=1, keepdims=True)
    own_b = jnp.broadcast_to(own, (128, 128))
    own_col = jnp.sum(jnp.where(row == lane, own_b, 0), axis=1, keepdims=True)
    earlier = jnp.where((own_col == own_b) & (row < lane), 1, 0)
    nth_own = jnp.sum(earlier, axis=0, keepdims=True)
    wet = own < DEVICES
    target = jnp.where(wet, 2 * own + nth_own, -1)
    total = jnp.broadcast_to(total, (1, 128))
    rows = jnp.concatenate([arrival, target, block_row, block_col, total, total, total, total], axis=0)
    pick = jnp.where((lane // 8 == row) & (jnp.broadcast_to(wet, (128, 128))), 1.0, 0.0)[:BLOCK_ROWS]
    lane2 = lax.broadcasted_iota(jnp.int32, (128, TILE_COLS), 1)
    row2 = lax.broadcasted_iota(jnp.int32, (128, TILE_COLS), 0)
    spread = (row2 % 8 == lane2 // ABLOCK).astype(BF16)
    return rows, _mm(pick.astype(BF16), spread)


def _pack_kernel(
    dev_s, sens_s, owners_r, own_r, air_r, low_r, marine_r, back_r, msg_r, idx_r, wet_r, field_s, home_s, idx_s, copy_sem
):
    b = pl.program_id(0)

    @pl.when(b == 0)
    def _():
        rows, wet = _index_rows(owners_r[...], own_r[...].reshape(1, 128), dev_s[0])
        idx_r[...] = rows
        wet_r[...] = wet
        copy = pltpu.make_async_copy(idx_r, idx_s, copy_sem)
        copy.start()
        for j in range(8):
            start = 1152 * (j // 4) + 256 * (j % 4)
            hi, lo = _hilo(marine_r[:, start : start + 384])
            part = (_mm(hi, back_r[j % 4]) + _mm(lo, back_r[j % 4])) * (1.0 / 9.0)
            home_s[pl.ds(j, SLOTS, stride=8), :] = part
        copy.wait()
        held = idx_s[4, 0]

        def put(s, carry):
            @pl.when(s < held)
            def _():
                at = pl.multiple_of(s * 8, 8)
                msg_r[idx_s[0, s], 64:72, :] = home_s[pl.ds(at, 8), :].astype(BF16)

            return carry

        lax.fori_loop(0, SLOTS, put, 0, unroll=8)

    group = _lane_group()
    low = low_r[0]
    for f in range(FIELDS):
        value = air_r[f].astype(F32) + sens_s[f] * low
        for h in range(2):
            field_s[h, 32 * f : 32 * f + 32, :] = value[:, 128 * h : 128 * h + 128]
    for h in range(2):
        out = [[] for _ in range(4)]
        for j in range(8):
            v = [field_s[h, pl.ds(4 * j + k, 8, stride=32), :] for k in range(4)]
            for c, w in enumerate(_swap_groups(v, group)):
                out[c].append(w)
        for c in range(4):
            target = idx_s[1, b * 8 + 4 * h + c]
            packed = jnp.concatenate(out[c], axis=0).astype(BF16)

            @pl.when(target >= 0)
            def _():
                msg_r[target, 0:64, :] = packed


def _pack(dev, sens, owners, own, air, model, marine, back):
    return pl.pallas_call(
        _pack_kernel,
        grid_spec=pltpu.PrefetchScalarGridSpec(
            num_scalar_prefetch=2,
            grid=(BLOCK_ROWS,),
            in_specs=[
                pl.BlockSpec((128, 128), lambda b, *_: (0, 0)),
                pl.BlockSpec((1, 1, 128), lambda b, d, s: (d[0], 0, 0)),
                pl.BlockSpec((FIELDS, ABLOCK, TILE_COLS), lambda b, *_: (0, b, 0)),
                pl.BlockSpec((1, ABLOCK, TILE_COLS), lambda b, *_: (LEVELS - 1, b, 0)),
                pl.BlockSpec((SLOTS, OCELLS), lambda b, *_: (0, 0)),
                pl.BlockSpec((4, 384, 128), lambda b, *_: (0, 0, 0)),
            ],
            out_specs=[
                pl.BlockSpec((2 * DEVICES, MSG_ROWS, 128), lambda b, *_: (0, 0, 0)),
                pl.BlockSpec((8, 128), lambda b, *_: (0, 0)),
                pl.BlockSpec((BLOCK_ROWS, TILE_COLS), lambda b, *_: (0, 0)),
            ],
            scratch_shapes=[
                pltpu.VMEM((2, FIELDS * ABLOCK, 128), F32),
                pltpu.VMEM((SLOTS * 8, 128), F32),
                pltpu.SMEM((8, 128), jnp.int32),
                pltpu.SemaphoreType.DMA(()),
            ],
        ),
        out_shape=[
            jax.ShapeDtypeStruct((2 * DEVICES, MSG_ROWS, 128), BF16),
            jax.ShapeDtypeStruct((8, 128), jnp.int32),
            jax.ShapeDtypeStruct((BLOCK_ROWS, TILE_COLS), F32),
        ],
        name="pack",
    )(dev, sens, owners, own, air, model, marine, back)


def _analyse_kernel(pos_s, model_r, forcing_r, rows_r, cols_r, out_r):
    d = forcing_r[0] - model_r[0]
    hi, lo = _hilo(d)
    along = _mm(hi, cols_r[...]) + _mm(lo, cols_r[...])
    along = along + pltpu.roll(along, 64, 1)
    mean = jnp.sum(d, axis=1, keepdims=True) * (1.0 / 64.0)
    lane = lax.broadcasted_iota(jnp.int32, (TILE_ROWS, 128), 1)
    along = jnp.where(lane < 64, along, jnp.where(lane == 64, mean, 0.0))
    hi, lo = _hilo(along)
    contract = (((0,), (0,)), ((), ()))
    both = lax.dot_general(rows_r[...], hi, contract, preferred_element_type=F32) + lax.dot_general(
        rows_r[...], lo, contract, preferred_element_type=F32
    )
    out_r[0:64, :] = both[0:64] + both[64:128]
    mean = jnp.sum(along, axis=0, keepdims=True) * (1.0 / 64.0)
    row = lax.broadcasted_iota(jnp.int32, (8, 128), 0)
    out_r[64:72, :] = jnp.where(row == 0, jnp.broadcast_to(mean, (8, 128)), 0.0)


def _analyse(pos, model, forcing, basis):
    return pl.pallas_call(
        _analyse_kernel,
        grid_spec=pltpu.PrefetchScalarGridSpec(
            num_scalar_prefetch=1,
            grid=(LEVELS,),
            in_specs=[
                pl.BlockSpec((1, TILE_ROWS, TILE_COLS), lambda l, p: (l, 0, 0)),
                pl.BlockSpec((1, TILE_ROWS, TILE_COLS), lambda l, p: (l, 0, 0)),
                pl.BlockSpec((TILE_ROWS, 128), lambda l, p: (p[0], 0)),
                pl.BlockSpec((TILE_COLS, 128), lambda l, p: (p[1], 0)),
            ],
            out_specs=pl.BlockSpec((CROWS, 128), lambda l, p: (l, 0)),
        ),
        out_shape=jax.ShapeDtypeStruct((LEVELS * CROWS, 128), F32),
        name="analyse",
    )(pos, model, forcing, basis, basis)


def _nudge_kernel(
    pos_s, strength_s, sens_s, warm_s, coef_r, rows_r, cols_r, model_r, air_r, land_r, wet_r, out_r, base_r, cols_s
):
    step = pl.program_id(0)
    lane = lax.broadcasted_iota(jnp.int32, (CROWS, 128), 1)

    @pl.when(step == 0)
    def _():
        contract = (((1,), (1,)), ((), ()))
        cols = cols_r[...]
        for l in range(LEVELS):
            coef = coef_r[CROWS * l : CROWS * l + CROWS, :]
            modes = jnp.where(lane < 64, coef, 0.0)
            hi, lo = _hilo(modes + pltpu.roll(modes, 64, 1))
            low, _ = _hilo(modes - jnp.where(lane < 64, hi.astype(F32), 0.0))
            t = lax.dot_general(hi, cols, contract, preferred_element_type=F32) + lax.dot_general(
                low, cols, contract, preferred_element_type=F32
            )
            mean = jnp.sum(jnp.where(lane == 64, coef, 0.0), axis=1, keepdims=True) * (1.0 / 64.0)
            t = (t + mean) * strength_s[l]
            hi, lo = _hilo(t[0:64])
            cols_s[l, 0:64, :] = hi
            cols_s[l, 64:128, :] = hi
            cols_s[l, 128:192, :] = lo
            cols_s[l, 192:256, :] = jnp.broadcast_to((t[64:72] * (1.0 / 64.0))[0:1], (64, TILE_COLS)).astype(BF16)
            c = t[64:65] * (1.0 / 64.0)
            chi, clo = _hilo(c)
            r = lax.broadcasted_iota(jnp.int32, (64, TILE_COLS), 0)
            full = jnp.where(r == 0, chi.astype(F32), jnp.where(r == 1, clo.astype(F32), 0.0))
            cols_s[l, 192:256, :] = full.astype(BF16)

    n = model_r.shape[1]
    rows = rows_r[...]
    lane_n = lax.broadcasted_iota(jnp.int32, (n, 128), 1)
    second = jnp.where(lane_n < 64, rows.astype(F32), jnp.where(lane_n < 66, 1.0, 0.0)).astype(BF16)
    left = jnp.concatenate([rows, second], axis=1)
    low = None
    for l in range(LEVELS):
        low = model_r[l] + _mm(left, cols_s[l])
        out_r[l] = low
    heat = None
    gain = 0.0
    for f in range(FIELDS):
        part = warm_s[f] * air_r[f].astype(F32)
        heat = part if heat is None else heat + part
        gain = gain + warm_s[f] * sens_s[f]
    heat = heat + gain * low
    row = lax.broadcasted_iota(jnp.int32, (n, TILE_COLS), 0)
    col = lax.broadcasted_iota(jnp.int32, (n, TILE_COLS), 1)
    partner = jnp.where(col % 2 == 0, pltpu.roll(heat, TILE_COLS - 1, 1), pltpu.roll(heat, 1, 1))
    heat = heat * (5.0 / 6.0) + partner * (1.0 / 6.0)
    partner = jnp.where(row % 2 == 0, pltpu.roll(heat, n - 1, 0), pltpu.roll(heat, 1, 0))
    heat = heat * (5.0 / 6.0) + partner * (1.0 / 6.0)
    for i in range(n // ABLOCK):
        at = slice(ABLOCK * i, ABLOCK * i + ABLOCK)
        wet = wet_r[pl.ds(step * (n // ABLOCK) + i, 1), :] > 0.5
        base_r[at, :] = jnp.where(wet, heat[at], land_r[at, :].astype(F32))


def _nudge(pos, strength, sens, warm, coef, basis, model, air, land, wet):
    n = 128
    per = TILE_ROWS // n
    return pl.pallas_call(
        _nudge_kernel,
        grid_spec=pltpu.PrefetchScalarGridSpec(
            num_scalar_prefetch=4,
            grid=(per,),
            in_specs=[
                pl.BlockSpec((LEVELS * CROWS, 128), lambda i, *_: (0, 0)),
                pl.BlockSpec((n, 128), lambda i, p, *_: (p[0] * per + i, 0)),
                pl.BlockSpec((TILE_COLS, 128), lambda i, p, *_: (p[1], 0)),
                pl.BlockSpec((LEVELS, n, TILE_COLS), lambda i, *_: (0, i, 0)),
                pl.BlockSpec((FIELDS, n, TILE_COLS), lambda i, *_: (0, i, 0)),
                pl.BlockSpec((n, TILE_COLS), lambda i, *_: (i, 0)),
                pl.BlockSpec((BLOCK_ROWS, TILE_COLS), lambda i, *_: (0, 0)),
            ],
            out_specs=[
                pl.BlockSpec((LEVELS, n, TILE_COLS), lambda i, *_: (0, i, 0)),
                pl.BlockSpec((n, TILE_COLS), lambda i, *_: (i, 0)),
            ],
            scratch_shapes=[pltpu.VMEM((LEVELS, 256, TILE_COLS), BF16)],
        ),
        out_shape=[
            jax.ShapeDtypeStruct((LEVELS, TILE_ROWS, TILE_COLS), F32),
            jax.ShapeDtypeStruct((TILE_ROWS, TILE_COLS), F32),
        ],
        name="nudge",
    )(pos, strength, sens, warm, coef, basis, basis, model, air, land, wet)


def _regrid_tiles(get):
    for half in range(2):
        for t, first in enumerate(FWD_FIRST):
            j = 4 * half + first
            yield 1152 * half + 256 * t, min(256, 1152 - 256 * t), t, j


def _held_kernel(idx_s, strength_s, coef_r, basis_r, synth_r, turn_r, fwd_r, out_r, plain_s, other_s, mean_s, left_s, cell_s):
    lane = lax.broadcasted_iota(jnp.int32, (CROWS, 128), 1)
    coef = coef_r[...] * strength_s[LEVELS - 1]
    modes = jnp.where(lane < 64, coef, 0.0)
    modes = modes + pltpu.roll(modes, 64, 1)
    swapped = jnp.where(lane % 64 < 32, pltpu.roll(modes, 96, 1), pltpu.roll(modes, 32, 1))
    mean = jnp.sum(jnp.where(lane == 64, coef, 0.0), axis=1, keepdims=True) * (1.0 / 64.0)
    mean = jnp.broadcast_to(mean, (CROWS, 128))
    right = jnp.concatenate([modes, swapped, mean], axis=1)
    hi, lo = _hilo(right[0:64])
    weights = jnp.concatenate([hi, hi, lo, jnp.zeros_like(lo)], axis=0)
    const = right[64:65] * (1.0 / 64.0)
    chunk = 512
    for i in range(GRID // chunk):
        rows = basis_r[chunk * i : chunk * i + chunk, :]
        left = jnp.concatenate([rows, rows], axis=1)
        table = _mm(left, weights) + const
        for n, ref in enumerate((plain_s, other_s, mean_s)):
            ref[chunk * i : chunk * i + chunk, :] = table[:, 128 * n : 128 * n + 128]
    lane = lax.broadcasted_iota(jnp.int32, (8, 128), 1)
    low = lane < 64
    group = lane // 32

    def slot(s, carry):
        start = idx_s[2, s] * ABLOCK
        turn = turn_r[pl.ds(idx_s[3, s], 1), :]
        plains, others, means = (
            [ref[pl.ds(start + k, 8, stride=4), :] for k in range(4)] for ref in (plain_s, other_s, mean_s)
        )
        at = pl.multiple_of(s * 8, 8)
        for p in range(2):
            plain = jnp.where(low, plains[2 * p], plains[2 * p + 1])
            other = jnp.where(low, others[2 * p], others[2 * p + 1])
            left_s[pl.ds(at, 8), 128 * p : 128 * p + 128] = plain * turn[:, 0:128] + other * turn[:, 128:256]
        m = jnp.where(group == 0, means[0], means[1])
        m = jnp.where(group < 2, m, jnp.where(group == 2, means[2], means[3]))
        cell_s[pl.ds(at, 8), :] = m
        return carry

    lax.fori_loop(0, SLOTS, slot, 0, unroll=4)
    hi, lo = _hilo(left_s[...])
    both = _mm(hi, synth_r[...])
    cell_s[...] = cell_s[...] + both[:, 0:128] + both[:, 128:256] + _mm(lo, synth_r[:, 0:128])
    tiles = [_hilo(cell_s[pl.ds(j, SLOTS, stride=8), :]) for j in range(8)]
    for at, width, t, j in _regrid_tiles(None):
        w = fwd_r[t][:, 0:width]
        hi = jnp.concatenate([tiles[j][0], tiles[j + 1][0]], axis=1)
        lo = jnp.concatenate([tiles[j][1], tiles[j + 1][1]], axis=1)
        out_r[:, at : at + width] = _mm(hi, w) + _mm(lo, w)


def _held(idx, strength, coef, basis, synth, turn, fwd):
    whole = lambda *shape: pl.BlockSpec(shape, lambda i, *_: (0,) * len(shape))
    return pl.pallas_call(
        _held_kernel,
        grid_spec=pltpu.PrefetchScalarGridSpec(
            num_scalar_prefetch=2,
            grid=(1,),
            in_specs=[
                pl.BlockSpec((CROWS, 128), lambda i, *_: (LEVELS - 1, 0)),
                whole(GRID, 128),
                whole(256, 256),
                whole(128, 256),
                whole(5, 256, 256),
            ],
            out_specs=whole(SLOTS, OCELLS),
            scratch_shapes=[
                pltpu.VMEM((GRID, 128), F32),
                pltpu.VMEM((GRID, 128), F32),
                pltpu.VMEM((GRID, 128), F32),
                pltpu.VMEM((SLOTS * 8, 256), F32),
                pltpu.VMEM((SLOTS * 8, 128), F32),
            ],
        ),
        out_shape=jax.ShapeDtypeStruct((SLOTS, OCELLS), F32),
        name="held",
    )(idx, strength, coef, basis, synth, turn, fwd)


OCEAN_STEP = 32


def _column(s_ref, n):
    row = lax.broadcasted_iota(jnp.int32, (8, 128), 0)
    v = jnp.zeros((8, 128), F32)
    for f in range(n):
        v = jnp.where(row == f, s_ref[f], v)
    return v


def _sum_rows(v, row):
    for shift, bit in ((4, 4), (2, 2), (1, 1)):
        keep = (row & bit) == 0
        half = len(v) // 2
        v = [
            jnp.where(keep, v[i], pltpu.roll(v[i + half], shift, 0))
            + jnp.where(keep, pltpu.roll(v[i], 8 - shift, 0), v[i + half])
            for i in range(half)
        ]
    return v[0]


def _ocean_kernel(idx_s, sens_s, warm_s, *refs):
    blocks = refs[:OCEAN_STEP]
    incr_r, marine_r, fwd_r, flux_r, sst_r = refs[OCEAN_STEP:]
    step = pl.program_id(0)
    held = idx_s[4, 0] - step * OCEAN_STEP
    sens = _column(sens_s, FIELDS)
    warm = _column(warm_s, FIELDS)
    tiles = [
        jnp.concatenate([blocks[q][0, 8 * j : 8 * j + 8, :] for q in range(OCEAN_STEP)], axis=0) for j in range(8)
    ]
    row = lax.broadcasted_iota(jnp.int32, (8, 128), 0)
    for at, width, t, j in _regrid_tiles(None):
        y = _mm(jnp.concatenate([tiles[j], tiles[j + 1]], axis=1), fwd_r[t][:, 0:width])
        for u in range(width // 128):
            cols = slice(at + 128 * u, at + 128 * u + 128)
            for g in range(OCEAN_STEP // 8):
                heats = []
                for q in range(8):
                    s = 8 * g + q
                    value = y[8 * s : 8 * s + 8, 128 * u : 128 * u + 128]
                    value = value + sens * jnp.broadcast_to(incr_r[s : s + 1, cols], (8, 128))
                    value = jnp.where(s < held, value, 0.0).astype(BF16)
                    flux_r[s, :, cols] = value
                    heats.append(value.astype(F32) * warm)
                heat = _sum_rows(heats, row)
                keep = row + 8 * g < held
                sst_r[8 * g : 8 * g + 8, cols] = jnp.where(keep, marine_r[8 * g : 8 * g + 8, cols] + heat, 0.0)


def _ocean(idx, sens, warm, incoming, incr, marine, fwd):
    def block(q):
        return pl.BlockSpec((1, 64, 128), lambda i, idx, *_: (idx[0, i * OCEAN_STEP + q], 0, 0))

    rows = lambda: pl.BlockSpec((OCEAN_STEP, OCELLS), lambda i, *_: (i, 0))
    return pl.pallas_call(
        _ocean_kernel,
        grid_spec=pltpu.PrefetchScalarGridSpec(
            num_scalar_prefetch=3,
            grid=(SLOTS // OCEAN_STEP,),
            in_specs=[block(q) for q in range(OCEAN_STEP)]
            + [rows(), rows(), pl.BlockSpec((5, 256, 256), lambda i, *_: (0, 0, 0))],
            out_specs=[pl.BlockSpec((OCEAN_STEP, FIELDS, OCELLS), lambda i, *_: (i, 0, 0)), rows()],
        ),
        out_shape=[
            jax.ShapeDtypeStruct((SLOTS, FIELDS, OCELLS), BF16),
            jax.ShapeDtypeStruct((SLOTS, OCELLS), F32),
        ],
        name="ocean",
    )(idx, sens, warm, *([incoming] * OCEAN_STEP), incr, marine, fwd)


def _surface_kernel(idx_s, back_r, base_r, wet_r, out_r, cell_s):
    group = _lane_group()

    def rows(b, carry):
        for h in range(2):
            v = [back_r[jnp.maximum(idx_s[1, b * 8 + 4 * h + c], 0)].astype(F32) for c in range(4)]
            for k, w in enumerate(_swap_groups(v, group)):
                cell_s[h, pl.ds(k, 8, stride=4), :] = w
        at = pl.multiple_of(b * ABLOCK, ABLOCK)
        wet = wet_r[pl.ds(b, 1), :] > 0.5
        cells = jnp.concatenate([cell_s[0], cell_s[1]], axis=1)
        out_r[pl.ds(at, ABLOCK), :] = base_r[pl.ds(at, ABLOCK), :] + jnp.where(wet, cells, 0.0)
        return carry

    lax.fori_loop(0, BLOCK_ROWS, rows, 0, unroll=2)


def _surface(idx, incoming, base, wet):
    whole = lambda *shape: pl.BlockSpec(shape, lambda i, *_: (0,) * len(shape))
    return pl.pallas_call(
        _surface_kernel,
        grid_spec=pltpu.PrefetchScalarGridSpec(
            num_scalar_prefetch=1,
            grid=(1,),
            in_specs=[
                pl.BlockSpec((2 * DEVICES, 8, 128), lambda i, *_: (0, 8, 0)),
                whole(TILE_ROWS, TILE_COLS),
                whole(BLOCK_ROWS, TILE_COLS),
            ],
            out_specs=whole(TILE_ROWS, TILE_COLS),
            scratch_shapes=[pltpu.VMEM((2, ABLOCK, 128), F32)],
        ),
        out_shape=jax.ShapeDtypeStruct((TILE_ROWS, TILE_COLS), F32),
        name="surface",
    )(idx, incoming, base, wet)


def _shift(axis, to):
    return [(i, to(i)) for i in range(8 if axis == "ay" else 16)]


def _total(part):
    core = lax.axis_index("ay") % 2
    half = part.shape[0] // 2
    swap = _shift("ay", lambda i: i ^ 1)
    first, second = part[:half], part[half:]
    mine = jnp.where(core == 0, first, second)
    theirs = jnp.where(core == 0, second, first)
    mine = mine + lax.ppermute(theirs, "ay", swap)
    for axis, to in (
        ("ay", lambda d: lambda i: (i + 2 * d) % 8),
        ("ax", lambda d: lambda i: (i + 4 * d) % 16),
        ("ax", lambda d: lambda i: i // 4 * 4 + (i + d) % 4),
    ):
        others = [lax.ppermute(mine, axis, _shift(axis, to(d))) for d in (1, 3, 2)]
        mine = mine + others[0] + others[1] + others[2]
    theirs = lax.ppermute(mine, "ay", swap)
    return jnp.concatenate([jnp.where(core == 0, mine, theirs), jnp.where(core == 0, theirs, mine)], axis=0)


def body(
    gaseous_model,
    forcing_boundary,
    relaxation_strength_profile,
    bottom_exchange_aloft,
    exchange_bottom_sensitivity,
    terrain_skin_warmth,
    tile_processor_home,
    marine_place_warmth,
    warming_coefficient,
):
    basis, fwd, back, synth, turn = (jnp.asarray(t) for t in _tables())
    ay, ax = lax.axis_index("ay"), lax.axis_index("ax")
    dev = jnp.reshape(ay * N_AX + ax, (1,)).astype(jnp.int32)
    pos = jnp.stack([ay, ax]).astype(jnp.int32)
    owners = tile_processor_home.reshape(DEVICES, 128)
    message, idx, wet = _pack(
        dev,
        exchange_bottom_sensitivity,
        owners,
        tile_processor_home.reshape(DEVICES, 1, 128),
        bottom_exchange_aloft,
        gaseous_model,
        marine_place_warmth,
        back,
    )
    incoming = lax.all_to_all(
        message.reshape(DEVICES, 2 * MSG_ROWS, 128), ("ay", "ax"), split_axis=0, concat_axis=0, tiled=True
    ).reshape(2 * DEVICES, MSG_ROWS, 128)
    pos, _ = lax.optimization_barrier((pos, idx))
    part = _analyse(pos, gaseous_model, forcing_boundary, basis)
    coef = _total(part)
    state, base = _nudge(
        pos,
        relaxation_strength_profile,
        exchange_bottom_sensitivity,
        warming_coefficient,
        coef,
        basis,
        gaseous_model,
        bottom_exchange_aloft,
        terrain_skin_warmth,
        wet,
    )
    incr = _held(idx, relaxation_strength_profile, coef, basis, synth, turn, fwd)
    flux, sst = _ocean(
        idx, exchange_bottom_sensitivity, warming_coefficient, incoming, incr, marine_place_warmth, fwd
    )
    surface = _surface(idx, incoming, base, wet)
    return state, flux, sst, surface


def solution(mesh):
    return jax.shard_map(
        body,
        mesh=mesh,
        in_specs=(
            P(None, "ay", "ax"),
            P(None, "ay", "ax"),
            P(),
            P(None, "ay", "ax"),
            P(),
            P("ay", "ax"),
            P(),
            P(("ay", "ax"), None),
            P(),
        ),
        out_specs=(
            P(None, "ay", "ax"),
            P(("ay", "ax"), None, None),
            P(("ay", "ax"), None),
            P("ay", "ax"),
        ),
        check_vma=False,
    )
```

```python
import functools
import math

import jax
import jax.numpy as jnp
import numpy as np
from jax import lax
from jax.experimental import pallas as pl
from jax.experimental.pallas import tpu as pltpu
from jax.sharding import PartitionSpec as P

GRID = 4096
KMAX = 32
LEVELS = 4
FIELDS = 8
ABLOCK = 32
OBLOCK = 48
ACELLS = 1024
OCELLS = 2304
TILE_ROWS = 512
TILE_COLS = 256
BLOCK_ROWS = 16
BLOCK_COLS = 8
N_AX = 16
DEVICES = 128
SLOTS = 128
MODES = 64
CROWS = 72
MSG_ROWS = 72
F32 = jnp.float32
BF16 = jnp.bfloat16


def _split(x):
    hi = np.asarray(x, np.float32).astype(jnp.bfloat16)
    lo = (np.asarray(x, np.float64) - hi.astype(np.float64)).astype(jnp.bfloat16)
    return hi, lo


def _modes(points):
    k = np.arange(1, KMAX + 1)
    angle = (np.asarray(points)[:, None] * k[None, :] % GRID) * (2.0 * math.pi / GRID)
    factor = math.sqrt(2.0 / GRID)
    return np.concatenate([factor * np.cos(angle), factor * np.sin(angle)], axis=1)


def _intersection():
    o = np.arange(OBLOCK)[:, None]
    a = np.arange(ABLOCK)[None, :]
    return np.maximum(np.minimum(2 * o + 2, 3 * a + 3) - np.maximum(2 * o, 3 * a), 0).astype(np.float64)


@functools.cache
def _tables():
    hi, lo = _split(_modes(np.arange(GRID)))
    basis = np.concatenate([hi, lo], axis=1)
    inter = _intersection()
    kron = np.kron(inter, inter)
    forward = np.zeros((5, 256, 256), np.float32)
    for t, first in enumerate(FWD_FIRST):
        out = min(256, 1152 - 256 * t)
        forward[t, :, :out] = kron[256 * t : 256 * t + out, 128 * first : 128 * first + 256].T / 4.0
    back = np.zeros((4, 384, 128), np.float32)
    for j in range(4):
        back[j] = kron[256 * j : 256 * j + 384, 128 * j : 128 * j + 128]
    local = np.zeros((256, 128))
    for k in range(4):
        local[64 * k : 64 * k + 64, 32 * k : 32 * k + 32] = _modes(np.arange(ABLOCK)).T
    lhi, llo = _split(local)
    synth = np.concatenate([lhi, llo], axis=1)
    k = np.arange(1, KMAX + 1)
    alpha = (np.arange(128)[:, None] * ABLOCK * k[None, :] % GRID) * (2.0 * math.pi / GRID)
    c, s = np.cos(alpha), np.sin(alpha)
    turn = np.concatenate([c, c, c, c, s, -s, s, -s], axis=1).astype(np.float32)
    return basis, forward.astype(jnp.bfloat16), back.astype(jnp.bfloat16), synth, turn


FWD_FIRST = (0, 0, 1, 2, 2)


def _hilo(x):
    hi = x.astype(BF16)
    return hi, (x - hi.astype(F32)).astype(BF16)


def _mm(a, b):
    return jnp.dot(a, b, preferred_element_type=F32)


def _swap_groups(v, group):
    low2, even = group < 2, group % 2 == 0
    r = lambda x, n: pltpu.roll(x, n, 1)
    a0 = jnp.where(low2, v[0], r(v[2], 64))
    a2 = jnp.where(low2, r(v[0], 64), v[2])
    a1 = jnp.where(low2, v[1], r(v[3], 64))
    a3 = jnp.where(low2, r(v[1], 64), v[3])
    return (
        jnp.where(even, a0, r(a1, 32)),
        jnp.where(even, r(a0, 96), a1),
        jnp.where(even, a2, r(a3, 32)),
        jnp.where(even, r(a2, 96), a3),
    )


def _lane_group():
    return lax.broadcasted_iota(jnp.int32, (8, 128), 1) // 32


def _index_rows(owners, own, dev):
    lane = lax.broadcasted_iota(jnp.int32, (128, 128), 1)
    row = lax.broadcasted_iota(jnp.int32, (128, 128), 0)
    mine = owners == dev
    eq = mine.astype(F32)
    count = jnp.sum(eq, axis=1, keepdims=True)
    running = jnp.sum(_mm((row >= lane).astype(BF16), eq.astype(BF16)), axis=1, keepdims=True)
    before = (running <= lane.astype(F32)).astype(F32)
    tile = jnp.sum(before, axis=0, keepdims=True)
    base = jnp.sum(before * count, axis=0, keepdims=True)
    first = jnp.min(jnp.where(mine, lane, 127), axis=1, keepdims=True).astype(F32)
    last = jnp.max(jnp.where(mine, lane, 0), axis=1, keepdims=True).astype(F32)
    chosen = (row.astype(F32) == tile).astype(F32)
    first = jnp.sum(chosen * first, axis=0, keepdims=True)
    last = jnp.sum(chosen * last, axis=0, keepdims=True)
    tile_i = tile.astype(jnp.int32)
    nth = lane[:1] - base.astype(jnp.int32)
    held = tile_i < 128
    block = jnp.where(nth == 0, first, last).astype(jnp.int32)
    arrival = jnp.where(held, 2 * tile_i + nth, 0)
    block_row = jnp.where(held, (tile_i // N_AX) * BLOCK_ROWS + block // BLOCK_COLS, 0)
    block_col = jnp.where(held, (tile_i % N_AX) * BLOCK_COLS + block % BLOCK_COLS, 0)
    total = jnp.sum(held.astype(jnp.int32), axis=1, keepdims=True)
    own_b = jnp.broadcast_to(own, (128, 128))
    own_col = jnp.sum(jnp.where(row == lane, own_b, 0), axis=1, keepdims=True)
    earlier = jnp.where((own_col == own_b) & (row < lane), 1, 0)
    nth_own = jnp.sum(earlier, axis=0, keepdims=True)
    wet = own < DEVICES
    target = jnp.where(wet, 2 * own + nth_own, -1)
    total = jnp.broadcast_to(total, (1, 128))
    rows = jnp.concatenate([arrival, target, block_row, block_col, total, total, total, total], axis=0)
    pick = jnp.where((lane // 8 == row) & (jnp.broadcast_to(wet, (128, 128))), 1.0, 0.0)[:BLOCK_ROWS]
    lane2 = lax.broadcasted_iota(jnp.int32, (128, TILE_COLS), 1)
    row2 = lax.broadcasted_iota(jnp.int32, (128, TILE_COLS), 0)
    spread = (row2 % 8 == lane2 // ABLOCK).astype(BF16)
    return rows, _mm(pick.astype(BF16), spread)


def _pack_kernel(
    dev_s, sens_s, owners_r, own_r, air_r, low_r, marine_r, back_r, msg_r, idx_r, wet_r, field_s, home_s, idx_s, copy_sem
):
    b = pl.program_id(0)

    @pl.when(b == 0)
    def _():
        rows, wet = _index_rows(owners_r[...], own_r[...].reshape(1, 128), dev_s[0])
        idx_r[...] = rows
        wet_r[...] = wet
        copy = pltpu.make_async_copy(idx_r, idx_s, copy_sem)
        copy.start()
        for j in range(8):
            start = 1152 * (j // 4) + 256 * (j % 4)
            hi, lo = _hilo(marine_r[:, start : start + 384])
            part = (_mm(hi, back_r[j % 4]) + _mm(lo, back_r[j % 4])) * (1.0 / 9.0)
            home_s[pl.ds(j, SLOTS, stride=8), :] = part
        copy.wait()
        held = idx_s[4, 0]

        def put(s, carry):
            @pl.when(s < held)
            def _():
                at = pl.multiple_of(s * 8, 8)
                msg_r[idx_s[0, s], 64:72, :] = home_s[pl.ds(at, 8), :].astype(BF16)

            return carry

        lax.fori_loop(0, SLOTS, put, 0, unroll=8)

    group = _lane_group()
    low = low_r[0]
    for f in range(FIELDS):
        value = air_r[f].astype(F32) + sens_s[f] * low
        for h in range(2):
            field_s[h, 32 * f : 32 * f + 32, :] = value[:, 128 * h : 128 * h + 128]
    for h in range(2):
        out = [[] for _ in range(4)]
        for j in range(8):
            v = [field_s[h, pl.ds(4 * j + k, 8, stride=32), :] for k in range(4)]
            for c, w in enumerate(_swap_groups(v, group)):
                out[c].append(w)
        for c in range(4):
            target = idx_s[1, b * 8 + 4 * h + c]
            packed = jnp.concatenate(out[c], axis=0).astype(BF16)

            @pl.when(target >= 0)
            def _():
                msg_r[target, 0:64, :] = packed


def _pack(dev, sens, owners, own, air, model, marine, back):
    return pl.pallas_call(
        _pack_kernel,
        grid_spec=pltpu.PrefetchScalarGridSpec(
            num_scalar_prefetch=2,
            grid=(BLOCK_ROWS,),
            in_specs=[
                pl.BlockSpec((128, 128), lambda b, *_: (0, 0)),
                pl.BlockSpec((1, 1, 128), lambda b, d, s: (d[0], 0, 0)),
                pl.BlockSpec((FIELDS, ABLOCK, TILE_COLS), lambda b, *_: (0, b, 0)),
                pl.BlockSpec((1, ABLOCK, TILE_COLS), lambda b, *_: (LEVELS - 1, b, 0)),
                pl.BlockSpec((SLOTS, OCELLS), lambda b, *_: (0, 0)),
                pl.BlockSpec((4, 384, 128), lambda b, *_: (0, 0, 0)),
            ],
            out_specs=[
                pl.BlockSpec((2 * DEVICES, MSG_ROWS, 128), lambda b, *_: (0, 0, 0)),
                pl.BlockSpec((8, 128), lambda b, *_: (0, 0)),
                pl.BlockSpec((BLOCK_ROWS, TILE_COLS), lambda b, *_: (0, 0)),
            ],
            scratch_shapes=[
                pltpu.VMEM((2, FIELDS * ABLOCK, 128), F32),
                pltpu.VMEM((SLOTS * 8, 128), F32),
                pltpu.SMEM((8, 128), jnp.int32),
                pltpu.SemaphoreType.DMA(()),
            ],
        ),
        out_shape=[
            jax.ShapeDtypeStruct((2 * DEVICES, MSG_ROWS, 128), BF16),
            jax.ShapeDtypeStruct((8, 128), jnp.int32),
            jax.ShapeDtypeStruct((BLOCK_ROWS, TILE_COLS), F32),
        ],
        name="pack",
    )(dev, sens, owners, own, air, model, marine, back)


def _analyse_kernel(pos_s, model_r, forcing_r, rows_r, cols_r, out_r, left_s, right_s, core_s, border_s):
    l = pl.program_id(0)

    @pl.when(l == 0)
    def _():
        left_s[0:128, :] = jnp.transpose(rows_r[...].astype(F32)).astype(BF16)
        row = lax.broadcasted_iota(jnp.int32, (16, TILE_ROWS), 0)
        left_s[128:144, :] = jnp.where(row == 0, 1.0 / 64.0, 0.0).astype(BF16)
        right_s[:, 0:128] = cols_r[...]
        lane = lax.broadcasted_iota(jnp.int32, (TILE_COLS, 128), 1)
        right_s[:, 128:256] = jnp.where(lane == 0, 1.0 / 64.0, 0.0).astype(BF16)
        border_s[...] = jnp.zeros_like(border_s)
        core_s[...] = jnp.zeros_like(core_s)

    hi, lo = _hilo(forcing_r[0] - model_r[0])
    along = _mm(left_s[...], hi) + _mm(left_s[...], lo)
    along = jnp.concatenate([along[0:64] + along[64:128], along[128:136]], axis=0)
    hi, lo = _hilo(along)
    both = _mm(hi, right_s[...]) + _mm(lo, right_s[...])
    modes = both[:, 0:128]
    modes = modes + pltpu.roll(modes, 64, 1)
    lane = lax.broadcasted_iota(jnp.int32, (CROWS, 128), 1)
    means = jnp.broadcast_to(both[:, 128:129], (CROWS, 128))
    half = lane // 64 == l % 2
    at = pl.multiple_of(l // 2 * 64, 64)
    core_s[pl.ds(at, 64), :] = jnp.where(half[0:64], modes[0:64], core_s[pl.ds(at, 64), :])
    border_s[0:64, :] = jnp.where(lane[0:64] == l, means[0:64], border_s[0:64, :])
    row = lax.broadcasted_iota(jnp.int32, (8, 128), 0)
    old = border_s[64:72, :]
    const = jnp.broadcast_to(modes[64:65], (8, 128))
    corner = jnp.broadcast_to(means[64:65], (8, 128))
    old = jnp.where((row == l // 2) & half[0:8], const, old)
    border_s[64:72, :] = jnp.where((row == 2) & (lane[0:8] == l), corner, old)

    @pl.when(l == LEVELS - 1)
    def _():
        out_r[pl.ds(0, 128, stride=2), :] = core_s[...]
        out_r[pl.ds(1, 128, stride=2), :] = border_s[...]


def _unpack(coef_r, level):
    core = coef_r[pl.ds(128 * (level // 2), 64, stride=2), :]
    border = coef_r[pl.ds(1, 72, stride=2), :]
    lane = lax.broadcasted_iota(jnp.int32, (72, 128), 1)
    here = lane // 64 == level % 2
    core = jnp.where(here[0:64], core, 0.0)
    core = core + pltpu.roll(core, 64, 1)
    column = jnp.sum(jnp.where(lane == level, border, 0.0), axis=1, keepdims=True)
    row = jnp.where(here, border, 0.0)
    row = (row + pltpu.roll(row, 64, 1))[64 + level // 2 : 65 + level // 2]
    return core, column[0:64], row, column[66:67]


def _analyse(pos, model, forcing, basis):
    return pl.pallas_call(
        _analyse_kernel,
        grid_spec=pltpu.PrefetchScalarGridSpec(
            num_scalar_prefetch=1,
            grid=(LEVELS,),
            in_specs=[
                pl.BlockSpec((1, TILE_ROWS, TILE_COLS), lambda l, p: (l, 0, 0)),
                pl.BlockSpec((1, TILE_ROWS, TILE_COLS), lambda l, p: (l, 0, 0)),
                pl.BlockSpec((TILE_ROWS, 128), lambda l, p: (p[0], 0)),
                pl.BlockSpec((TILE_COLS, 128), lambda l, p: (p[1], 0)),
            ],
            out_specs=pl.BlockSpec((2 * DEVICES, 128), lambda l, p: (0, 0)),
            scratch_shapes=[
                pltpu.VMEM((144, TILE_ROWS), BF16),
                pltpu.VMEM((TILE_COLS, 256), BF16),
                pltpu.VMEM((128, 128), F32),
                pltpu.VMEM((128, 128), F32),
            ],
        ),
        out_shape=jax.ShapeDtypeStruct((2 * DEVICES, 128), F32),
        name="analyse",
    )(pos, model, forcing, basis, basis)


def _nudge_kernel(
    pos_s, strength_s, sens_s, warm_s, coef_r, rows_r, cols_r, model_r, air_r, land_r, wet_r, out_r, base_r, cols_s
):
    step = pl.program_id(0)
    lane = lax.broadcasted_iota(jnp.int32, (CROWS, 128), 1)

    @pl.when(step == 0)
    def _():
        contract = (((1,), (1,)), ((), ()))
        cols = cols_r[...]
        for l in range(LEVELS):
            modes, column, const, corner = _unpack(coef_r, l)
            parts = []
            for block, mean in ((modes, column), (jnp.broadcast_to(const, (8, 128)), corner)):
                hi, lo = _hilo(block)
                lo = jnp.where(lane[: block.shape[0]] < 64, lo.astype(F32), 0.0).astype(BF16)
                t = lax.dot_general(hi, cols, contract, preferred_element_type=F32) + lax.dot_general(
                    lo, cols, contract, preferred_element_type=F32
                )
                parts.append((t + mean * (1.0 / 64.0)) * strength_s[l])
            hi, lo = _hilo(parts[0])
            cols_s[l, 0:64, :] = hi
            cols_s[l, 64:128, :] = hi
            cols_s[l, 128:192, :] = lo
            hi, lo = _hilo(parts[1][0:1] * (1.0 / 64.0))
            r = lax.broadcasted_iota(jnp.int32, (64, TILE_COLS), 0)
            cols_s[l, 192:256, :] = jnp.where(r == 0, hi.astype(F32), jnp.where(r == 1, lo.astype(F32), 0.0)).astype(BF16)

    n = model_r.shape[1]
    rows = rows_r[...]
    lane_n = lax.broadcasted_iota(jnp.int32, (n, 128), 1)
    second = jnp.where(lane_n < 64, rows.astype(F32), jnp.where(lane_n < 66, 1.0, 0.0)).astype(BF16)
    left = jnp.concatenate([rows, second], axis=1)
    low = None
    for l in range(LEVELS):
        low = model_r[l] + _mm(left, cols_s[l])
        out_r[l] = low
    heat = None
    gain = 0.0
    for f in range(FIELDS):
        part = warm_s[f] * air_r[f].astype(F32)
        heat = part if heat is None else heat + part
        gain = gain + warm_s[f] * sens_s[f]
    heat = heat + gain * low
    row = lax.broadcasted_iota(jnp.int32, (n, TILE_COLS), 0)
    col = lax.broadcasted_iota(jnp.int32, (n, TILE_COLS), 1)
    partner = jnp.where(col % 2 == 0, pltpu.roll(heat, TILE_COLS - 1, 1), pltpu.roll(heat, 1, 1))
    heat = heat * (5.0 / 6.0) + partner * (1.0 / 6.0)
    partner = jnp.where(row % 2 == 0, pltpu.roll(heat, n - 1, 0), pltpu.roll(heat, 1, 0))
    heat = heat * (5.0 / 6.0) + partner * (1.0 / 6.0)
    for i in range(n // ABLOCK):
        at = slice(ABLOCK * i, ABLOCK * i + ABLOCK)
        wet = wet_r[pl.ds(step * (n // ABLOCK) + i, 1), :] > 0.5
        base_r[at, :] = jnp.where(wet, heat[at], land_r[at, :].astype(F32))


def _nudge(pos, strength, sens, warm, coef, basis, model, air, land, wet):
    n = 128
    per = TILE_ROWS // n
    return pl.pallas_call(
        _nudge_kernel,
        grid_spec=pltpu.PrefetchScalarGridSpec(
            num_scalar_prefetch=4,
            grid=(per,),
            in_specs=[
                pl.BlockSpec((2 * DEVICES, 128), lambda i, *_: (0, 0)),
                pl.BlockSpec((n, 128), lambda i, p, *_: (p[0] * per + i, 0)),
                pl.BlockSpec((TILE_COLS, 128), lambda i, p, *_: (p[1], 0)),
                pl.BlockSpec((LEVELS, n, TILE_COLS), lambda i, *_: (0, i, 0)),
                pl.BlockSpec((FIELDS, n, TILE_COLS), lambda i, *_: (0, i, 0)),
                pl.BlockSpec((n, TILE_COLS), lambda i, *_: (i, 0)),
                pl.BlockSpec((BLOCK_ROWS, TILE_COLS), lambda i, *_: (0, 0)),
            ],
            out_specs=[
                pl.BlockSpec((LEVELS, n, TILE_COLS), lambda i, *_: (0, i, 0)),
                pl.BlockSpec((n, TILE_COLS), lambda i, *_: (i, 0)),
            ],
            scratch_shapes=[pltpu.VMEM((LEVELS, 256, TILE_COLS), BF16)],
        ),
        out_shape=[
            jax.ShapeDtypeStruct((LEVELS, TILE_ROWS, TILE_COLS), F32),
            jax.ShapeDtypeStruct((TILE_ROWS, TILE_COLS), F32),
        ],
        name="nudge",
    )(pos, strength, sens, warm, coef, basis, basis, model, air, land, wet)


def _regrid_tiles(get):
    for half in range(2):
        for t, first in enumerate(FWD_FIRST):
            j = 4 * half + first
            yield 1152 * half + 256 * t, min(256, 1152 - 256 * t), t, j


def _held_kernel(idx_s, strength_s, coef_r, basis_r, synth_r, turn_r, fwd_r, out_r, plain_s, other_s, mean_s, left_s, cell_s):
    lane = lax.broadcasted_iota(jnp.int32, (64, 128), 1)
    strength = strength_s[LEVELS - 1]
    modes, column, row, corner = _unpack(coef_r, LEVELS - 1)

    def swap(x):
        return jnp.where(lane[: x.shape[0]] % 64 < 32, pltpu.roll(x, 96, 1), pltpu.roll(x, 32, 1))

    column = jnp.broadcast_to(column * (1.0 / 64.0), (64, 128))
    right = jnp.concatenate([modes, swap(modes), column], axis=1) * strength
    row = jnp.broadcast_to(row, (8, 128))
    corner = jnp.broadcast_to(corner * (1.0 / 64.0), (8, 128))
    const = jnp.concatenate([row, swap(row), corner], axis=1)[0:1] * (strength * (1.0 / 64.0))
    hi, lo = _hilo(right)
    weights = jnp.concatenate([hi, hi, lo, jnp.zeros_like(lo)], axis=0)
    chunk = 512
    for i in range(GRID // chunk):
        rows = basis_r[chunk * i : chunk * i + chunk, :]
        left = jnp.concatenate([rows, rows], axis=1)
        table = _mm(left, weights) + const
        for n, ref in enumerate((plain_s, other_s, mean_s)):
            ref[chunk * i : chunk * i + chunk, :] = table[:, 128 * n : 128 * n + 128]
    lane = lax.broadcasted_iota(jnp.int32, (8, 128), 1)
    low = lane < 64
    group = lane // 32

    def slot(s, carry):
        start = idx_s[2, s] * ABLOCK
        turn = turn_r[pl.ds(idx_s[3, s], 1), :]
        plains, others, means = (
            [ref[pl.ds(start + k, 8, stride=4), :] for k in range(4)] for ref in (plain_s, other_s, mean_s)
        )
        at = pl.multiple_of(s * 8, 8)
        for p in range(2):
            plain = jnp.where(low, plains[2 * p], plains[2 * p + 1])
            other = jnp.where(low, others[2 * p], others[2 * p + 1])
            left_s[pl.ds(at, 8), 128 * p : 128 * p + 128] = plain * turn[:, 0:128] + other * turn[:, 128:256]
        m = jnp.where(group == 0, means[0], means[1])
        m = jnp.where(group < 2, m, jnp.where(group == 2, means[2], means[3]))
        cell_s[pl.ds(at, 8), :] = m
        return carry

    lax.fori_loop(0, SLOTS, slot, 0, unroll=4)
    hi, lo = _hilo(left_s[...])
    both = _mm(hi, synth_r[...])
    cell_s[...] = cell_s[...] + both[:, 0:128] + both[:, 128:256] + _mm(lo, synth_r[:, 0:128])
    tiles = [_hilo(cell_s[pl.ds(j, SLOTS, stride=8), :]) for j in range(8)]
    for at, width, t, j in _regrid_tiles(None):
        w = fwd_r[t][:, 0:width]
        hi = jnp.concatenate([tiles[j][0], tiles[j + 1][0]], axis=1)
        lo = jnp.concatenate([tiles[j][1], tiles[j + 1][1]], axis=1)
        out_r[:, at : at + width] = _mm(hi, w) + _mm(lo, w)


def _held(idx, strength, coef, basis, synth, turn, fwd):
    whole = lambda *shape: pl.BlockSpec(shape, lambda i, *_: (0,) * len(shape))
    return pl.pallas_call(
        _held_kernel,
        grid_spec=pltpu.PrefetchScalarGridSpec(
            num_scalar_prefetch=2,
            grid=(1,),
            in_specs=[
                whole(2 * DEVICES, 128),
                whole(GRID, 128),
                whole(256, 256),
                whole(128, 256),
                whole(5, 256, 256),
            ],
            out_specs=whole(SLOTS, OCELLS),
            scratch_shapes=[
                pltpu.VMEM((GRID, 128), F32),
                pltpu.VMEM((GRID, 128), F32),
                pltpu.VMEM((GRID, 128), F32),
                pltpu.VMEM((SLOTS * 8, 256), F32),
                pltpu.VMEM((SLOTS * 8, 128), F32),
            ],
        ),
        out_shape=jax.ShapeDtypeStruct((SLOTS, OCELLS), F32),
        name="held",
    )(idx, strength, coef, basis, synth, turn, fwd)


OCEAN_STEP = 32


def _column(s_ref, n):
    row = lax.broadcasted_iota(jnp.int32, (8, 128), 0)
    v = jnp.zeros((8, 128), F32)
    for f in range(n):
        v = jnp.where(row == f, s_ref[f], v)
    return v


def _sum_rows(v, row):
    for shift, bit in ((4, 4), (2, 2), (1, 1)):
        keep = (row & bit) == 0
        half = len(v) // 2
        v = [
            jnp.where(keep, v[i], pltpu.roll(v[i + half], shift, 0))
            + jnp.where(keep, pltpu.roll(v[i], 8 - shift, 0), v[i + half])
            for i in range(half)
        ]
    return v[0]


def _ocean_kernel(idx_s, sens_s, warm_s, *refs):
    blocks = refs[:OCEAN_STEP]
    incr_r, marine_r, fwd_r, flux_r, sst_r = refs[OCEAN_STEP:]
    step = pl.program_id(0)
    held = idx_s[4, 0] - step * OCEAN_STEP
    sens = _column(sens_s, FIELDS)
    warm = _column(warm_s, FIELDS)
    tiles = [
        jnp.concatenate([blocks[q][0, 8 * j : 8 * j + 8, :] for q in range(OCEAN_STEP)], axis=0) for j in range(8)
    ]
    row = lax.broadcasted_iota(jnp.int32, (8, 128), 0)
    for at, width, t, j in _regrid_tiles(None):
        y = _mm(jnp.concatenate([tiles[j], tiles[j + 1]], axis=1), fwd_r[t][:, 0:width])
        for u in range(width // 128):
            cols = slice(at + 128 * u, at + 128 * u + 128)
            for g in range(OCEAN_STEP // 8):
                heats = []
                for q in range(8):
                    s = 8 * g + q
                    value = y[8 * s : 8 * s + 8, 128 * u : 128 * u + 128]
                    value = value + sens * jnp.broadcast_to(incr_r[s : s + 1, cols], (8, 128))
                    value = jnp.where(s < held, value, 0.0).astype(BF16)
                    flux_r[s, :, cols] = value
                    heats.append(value.astype(F32) * warm)
                heat = _sum_rows(heats, row)
                keep = row + 8 * g < held
                sst_r[8 * g : 8 * g + 8, cols] = jnp.where(keep, marine_r[8 * g : 8 * g + 8, cols] + heat, 0.0)


def _ocean(idx, sens, warm, incoming, incr, marine, fwd):
    def block(q):
        return pl.BlockSpec((1, 64, 128), lambda i, idx, *_: (idx[0, i * OCEAN_STEP + q], 0, 0))

    rows = lambda: pl.BlockSpec((OCEAN_STEP, OCELLS), lambda i, *_: (i, 0))
    return pl.pallas_call(
        _ocean_kernel,
        grid_spec=pltpu.PrefetchScalarGridSpec(
            num_scalar_prefetch=3,
            grid=(SLOTS // OCEAN_STEP,),
            in_specs=[block(q) for q in range(OCEAN_STEP)]
            + [rows(), rows(), pl.BlockSpec((5, 256, 256), lambda i, *_: (0, 0, 0))],
            out_specs=[pl.BlockSpec((OCEAN_STEP, FIELDS, OCELLS), lambda i, *_: (i, 0, 0)), rows()],
        ),
        out_shape=[
            jax.ShapeDtypeStruct((SLOTS, FIELDS, OCELLS), BF16),
            jax.ShapeDtypeStruct((SLOTS, OCELLS), F32),
        ],
        name="ocean",
    )(idx, sens, warm, *([incoming] * OCEAN_STEP), incr, marine, fwd)


def _surface_kernel(idx_s, back_r, base_r, wet_r, out_r, cell_s):
    group = _lane_group()

    def rows(b, carry):
        for h in range(2):
            v = [back_r[jnp.maximum(idx_s[1, b * 8 + 4 * h + c], 0)].astype(F32) for c in range(4)]
            for k, w in enumerate(_swap_groups(v, group)):
                cell_s[h, pl.ds(k, 8, stride=4), :] = w
        at = pl.multiple_of(b * ABLOCK, ABLOCK)
        wet = wet_r[pl.ds(b, 1), :] > 0.5
        cells = jnp.concatenate([cell_s[0], cell_s[1]], axis=1)
        out_r[pl.ds(at, ABLOCK), :] = base_r[pl.ds(at, ABLOCK), :] + jnp.where(wet, cells, 0.0)
        return carry

    lax.fori_loop(0, BLOCK_ROWS, rows, 0, unroll=2)


def _surface(idx, incoming, base, wet):
    whole = lambda *shape: pl.BlockSpec(shape, lambda i, *_: (0,) * len(shape))
    return pl.pallas_call(
        _surface_kernel,
        grid_spec=pltpu.PrefetchScalarGridSpec(
            num_scalar_prefetch=1,
            grid=(1,),
            in_specs=[
                pl.BlockSpec((2 * DEVICES, 8, 128), lambda i, *_: (0, 8, 0)),
                whole(TILE_ROWS, TILE_COLS),
                whole(BLOCK_ROWS, TILE_COLS),
            ],
            out_specs=whole(TILE_ROWS, TILE_COLS),
            scratch_shapes=[pltpu.VMEM((2, ABLOCK, 128), F32)],
        ),
        out_shape=jax.ShapeDtypeStruct((TILE_ROWS, TILE_COLS), F32),
        name="surface",
    )(idx, incoming, base, wet)


def _exchange(x):
    return lax.all_to_all(x, ("ay", "ax"), split_axis=0, concat_axis=0, tiled=True)


def body(
    gaseous_model,
    forcing_boundary,
    relaxation_strength_profile,
    bottom_exchange_aloft,
    exchange_bottom_sensitivity,
    terrain_skin_warmth,
    tile_processor_home,
    marine_place_warmth,
    warming_coefficient,
):
    basis, fwd, back, synth, turn = (jnp.asarray(t) for t in _tables())
    ay, ax = lax.axis_index("ay"), lax.axis_index("ax")
    dev = jnp.reshape(ay * N_AX + ax, (1,)).astype(jnp.int32)
    pos = jnp.stack([ay, ax]).astype(jnp.int32)
    owners = tile_processor_home.reshape(DEVICES, 128)
    part = _analyse(pos, gaseous_model, forcing_boundary, basis)
    part = _exchange(part.reshape(DEVICES, 2, 128))
    message, idx, wet = _pack(
        dev,
        exchange_bottom_sensitivity,
        owners,
        tile_processor_home.reshape(DEVICES, 1, 128),
        bottom_exchange_aloft,
        gaseous_model,
        marine_place_warmth,
        back,
    )
    total = jnp.broadcast_to(jnp.sum(part, axis=0, keepdims=True), (DEVICES, 2, 128))
    coef = _exchange(total)
    message, coef = lax.optimization_barrier((message, coef))
    coef = coef.reshape(2 * DEVICES, 128)
    incoming = _exchange(message.reshape(DEVICES, 2 * MSG_ROWS, 128)).reshape(2 * DEVICES, MSG_ROWS, 128)
    state, base = _nudge(
        pos,
        relaxation_strength_profile,
        exchange_bottom_sensitivity,
        warming_coefficient,
        coef,
        basis,
        gaseous_model,
        bottom_exchange_aloft,
        terrain_skin_warmth,
        wet,
    )
    incr = _held(idx, relaxation_strength_profile, coef, basis, synth, turn, fwd)
    flux, sst = _ocean(
        idx, exchange_bottom_sensitivity, warming_coefficient, incoming, incr, marine_place_warmth, fwd
    )
    surface = _surface(idx, incoming, base, wet)
    return state, flux, sst, surface


def solution(mesh):
    return jax.shard_map(
        body,
        mesh=mesh,
        in_specs=(
            P(None, "ay", "ax"),
            P(None, "ay", "ax"),
            P(),
            P(None, "ay", "ax"),
            P(),
            P("ay", "ax"),
            P(),
            P(("ay", "ax"), None),
            P(),
        ),
        out_specs=(
            P(None, "ay", "ax"),
            P(("ay", "ax"), None, None),
            P(("ay", "ax"), None),
            P("ay", "ax"),
        ),
        check_vma=False,
    )
```
